32 devices in a mesh: patch: 2 (over core), theta: 4 (over z), phi: 4 (over y, x).
Axes of the slice: x: 2, y: 2, z: 4, core: 2. Of those that a mesh axis runs over, the one named last changes fastest.
Arguments:
- density: float32 [2, 16, 64, 512], P('patch', None, 'theta', 'phi'), may hold values from 0.5 to 2
- velocity: float32 [2, 3, 16, 64, 512], P('patch', None, None, 'theta', 'phi'), may hold values from -3 to 3
- magnetic: float32 [2, 3, 16, 64, 512], P('patch', None, None, 'theta', 'phi'), may hold values from -3 to 3
- pressure: float32 [2, 16, 64, 512], P('patch', None, 'theta', 'phi'), may hold values from 0.5 to 2
- send_row: int32 [2, 4, 4, 144], P('patch', 'theta', 'phi'), may hold values from 0 to 14
- send_col: int32 [2, 4, 4, 144], P('patch', 'theta', 'phi'), may hold values from 0 to 126
- send_weight: float32 [2, 4, 4, 2, 144], P('patch', 'theta', 'phi'), may hold values from 0 to 1
- send_turn: float32 [2, 4, 4, 144], P('patch', 'theta', 'phi'), may hold values from -3.140625 to 3.140625
- send_dest: int32 [2, 4, 4, 144], P('patch', 'theta', 'phi'), may hold values from 0 to 1152, as said below
Outputs:
- new_density: float32 [2, 16, 64, 512], P('patch', None, 'theta', 'phi')
- new_velocity: float32 [2, 3, 16, 64, 512], P('patch', None, None, 'theta', 'phi')
- new_magnetic: float32 [2, 3, 16, 64, 512], P('patch', None, None, 'theta', 'phi')
- new_pressure: float32 [2, 16, 64, 512], P('patch', None, 'theta', 'phi')
The draws below stay inside these ranges and needn't reach their ends.
Inputs may be any that keep to these rules, and one draw needn't show every extreme that they name: `send_dest`: each ghost point m < 1152 of a patch is named by exactly one slot of the other patch's tiles; unused slots hold 1152. Used slots lie only in tiles of the first and last tile rows and tile columns of a patch, and their donor cells lie within min(16, 128) cells of the patch's outer edge; the four corner tiles use all 144 slots, every other tile fewer.
All inputs are finite; a program needn't handle non-finite values.
Results may differ from the reference program's by a relative error of at most 0.00008.
Values sent between devices are 32-bit elements; how exact they have to be, the bound alone decides.
A program may use at most 64 MiB of HBM per device.

```python
import math
import jax
import jax.numpy as jnp
from jax import lax

NR = 16
CT = 16
CP = 128
NTH = 64
NPH = 512
BORDER = 1152
SEND = 144
N_THETA = 4
N_PHI = 4


def donor_layout(key):
    row_tiles = NTH // CT
    col_tiles = NPH // CP
    tile_count = row_tiles * col_tiles
    slot_count = tile_count * SEND

    def one_patch(patch_key):
        inset_key, order_key, row_key, col_key = jax.random.split(patch_key, 4)
        ghost = jnp.arange(BORDER, dtype=jnp.int32)
        side = jnp.where(ghost < NPH, 0, jnp.where(ghost < 2 * NPH, 1, jnp.where(ghost < 2 * NPH + NTH, 2, 3)))
        offset = jnp.where(side == 0, 0, jnp.where(side == 1, NPH, jnp.where(side == 2, 2 * NPH, 2 * NPH + NTH)))
        along = ghost - offset
        depth = jax.random.randint(inset_key, (BORDER,), 0, min(CT, CP) - 1, dtype=jnp.int32)
        down_row = jnp.minimum(along * NTH // NPH, NTH - 2)
        up_row = jnp.minimum(jnp.maximum(NPH - 1 - along, 0) * NTH // NPH, NTH - 2)
        fwd_col = jnp.minimum(along * NPH // NTH, NPH - 2)
        back_col = jnp.minimum(jnp.maximum(NTH - 1 - along, 0) * NPH // NTH, NPH - 2)
        row_cell = jnp.where(side == 0, down_row, jnp.where(side == 1, up_row, jnp.where(side == 2, depth, NTH - 2 - depth)))
        col_cell = jnp.where(side == 0, depth, jnp.where(side == 1, NPH - 2 - depth, jnp.where(side == 2, fwd_col, back_col)))
        tile_row = row_cell // CT
        tile_col = col_cell // CP
        local_row = jnp.minimum(row_cell - tile_row * CT, CT - 2)
        local_col = jnp.minimum(col_cell - tile_col * CP, CP - 2)
        tile = tile_row * col_tiles + tile_col
        priority = jax.random.permutation(order_key, BORDER).astype(jnp.int32)
        order = jnp.argsort(tile * BORDER + priority, stable=True).astype(jnp.int32)
        sorted_tile = tile[order]
        counts = jnp.zeros((tile_count,), jnp.int32).at[tile].add(1)
        starts = jnp.cumsum(counts).astype(jnp.int32) - counts
        slot = jnp.arange(BORDER, dtype=jnp.int32) - starts[sorted_tile]
        flat = sorted_tile * SEND + slot
        target = jnp.full((slot_count,), BORDER, dtype=jnp.int32).at[flat].set(order)
        rows = jax.random.randint(row_key, (slot_count,), 0, CT - 1, dtype=jnp.int32).at[flat].set(local_row[order])
        cols = jax.random.randint(col_key, (slot_count,), 0, CP - 1, dtype=jnp.int32).at[flat].set(local_col[order])
        shape = (row_tiles, col_tiles, SEND)
        return (target.reshape(shape), rows.reshape(shape), cols.reshape(shape))
    first = one_patch(jax.random.fold_in(key, 11))
    second = one_patch(jax.random.fold_in(key, 23))
    return (jnp.stack([first[0], second[0]]), jnp.stack([first[1], second[1]]), jnp.stack([first[2], second[2]]))


def draw_send_dest(key, part):
    return donor_layout(key)[0]


def draw_send_row(key, part):
    return donor_layout(key)[1]


def draw_send_col(key, part):
    return donor_layout(key)[2]


def steps_of(own_key, extent, cuts, low, top_value):
    loudness, own = 1.0, jax.random.fold_in(own_key, 6)
    for dim, shards_of in cuts:
        heights = jnp.exp(jax.random.uniform(jax.random.fold_in(own, dim), (shards_of,), jnp.float32, low / len(cuts), top_value / len(cuts)))
        loudness = loudness * jnp.repeat(heights, extent[dim] // shards_of).reshape([-1 if axis == dim else 1 for axis in range(len(extent))])
    return loudness


def gaussian(rng, extent, deviation, most, cuts=(), kind=jnp.bfloat16):
    entries = deviation * jax.random.normal(rng, extent, jnp.float32)
    if cuts:
        entries = entries * steps_of(rng, extent, cuts, -0.22, 0.18)
    return jnp.clip(entries, -most, most).astype(kind)


def setup_inputs(seed: int = 0) -> dict:
    splits = jax.random.split(jax.random.key(seed), 10)
    return {
        "density": jnp.clip(jnp.exp(math.log(2.0) - 1.3862944 * jax.random.uniform(splits[0], (2, NR, NTH, NPH), jnp.float32) ** steps_of(splits[0], (2, NR, NTH, NPH), ((0, 2), (2, 4), (3, 4)), -0.2, 0.2)), 0.5, 2.0),
        "velocity": gaussian(splits[1], (2, 3, NR, NTH, NPH), 0.5, 3.0, ((0, 2), (3, 4), (4, 4)), jnp.float32),
        "magnetic": gaussian(splits[2], (2, 3, NR, NTH, NPH), 0.5, 3.0, ((0, 2), (3, 4), (4, 4)), jnp.float32),
        "pressure": jnp.clip(jnp.exp(math.log(2.0) - 1.3862944 * jax.random.uniform(splits[3], (2, NR, NTH, NPH), jnp.float32) ** steps_of(splits[3], (2, NR, NTH, NPH), ((0, 2), (2, 4), (3, 4)), -0.2, 0.2)), 0.5, 2.0),
        "send_row": draw_send_row(jax.random.fold_in(splits[9], 71), 0),
        "send_col": draw_send_col(jax.random.fold_in(splits[9], 71), 0),
        "send_weight": jnp.clip(1.0 * jax.random.uniform(splits[6], (2, N_THETA, N_PHI, 2, SEND), jnp.float32) ** steps_of(splits[6], (2, N_THETA, N_PHI, 2, SEND), ((0, 2), (1, 4), (2, 4)), -0.2, 0.2), 0.0, 1.0),
        "send_turn": jnp.clip(jax.random.uniform(splits[7], (2, N_THETA, N_PHI, SEND), jnp.float32, -3.140625, 3.140625), -3.140625, 3.140625),
        "send_dest": draw_send_dest(jax.random.fold_in(splits[9], 71), 0),
    }


GAMMA = 5.0 / 3.0
R_BASE = 0.6
DR_STEP = 0.65 / 64.0
COURANT = 0.4
DIFFUSE = 0.4


def grid_constants(total_theta, total_phi):
    d_theta = 0.5 * math.pi / total_theta
    d_phi = 1.5 * math.pi / total_phi
    r_low = R_BASE + 0.5 * DR_STEP
    inv_r = 1.0 / DR_STEP
    inv_t = 1.0 / (r_low * d_theta)
    inv_p = 1.0 / (r_low * math.sin(0.25 * math.pi) * d_phi)
    dt_step = COURANT / (inv_r + inv_t + inv_p)
    diffusivity = DIFFUSE / (dt_step * (inv_r * inv_r + inv_t * inv_t + inv_p * inv_p))
    return d_theta, d_phi, dt_step, diffusivity


def bilinear(low_low, low_high, high_low, high_high, weight_row, weight_col):
    return (1.0 - weight_row) * ((1.0 - weight_col) * low_low + weight_col * low_high) + weight_row * ((1.0 - weight_col) * high_low + weight_col * high_high)


def turn_frame(blended, turn):
    cos_t = jnp.cos(turn)
    sin_t = jnp.sin(turn)
    flow_t = cos_t * blended[2] + sin_t * blended[3]
    flow_p = cos_t * blended[3] - sin_t * blended[2]
    field_t = cos_t * blended[5] + sin_t * blended[6]
    field_p = cos_t * blended[6] - sin_t * blended[5]
    return jnp.stack([blended[0], blended[1], flow_t, flow_p, blended[4], field_t, field_p, blended[7]])


def advance(padded, radius, sin_theta, d_theta, d_phi, dt_step, diffusivity):
    levels = padded.shape[1] - 2
    tile_rows = padded.shape[2] - 2
    tile_cols = padded.shape[3] - 2
    radial_h = 1.0 / DR_STEP
    colat_h = 1.0 / (radius[:, None, None] * d_theta)
    lon_h = 1.0 / (radius[:, None, None] * sin_theta[None, :, None] * d_phi)

    def shifted(field, step_r, step_t, step_p):
        return field[..., 1 + step_r:1 + step_r + levels, 1 + step_t:1 + step_t + tile_rows, 1 + step_p:1 + step_p + tile_cols]

    def radial_diff(field):
        return (shifted(field, 1, 0, 0) - shifted(field, -1, 0, 0)) * (0.5 * radial_h)

    def colat_diff(field):
        return (shifted(field, 0, 1, 0) - shifted(field, 0, -1, 0)) * (0.5 * colat_h)

    def lon_diff(field):
        return (shifted(field, 0, 0, 1) - shifted(field, 0, 0, -1)) * (0.5 * lon_h)

    def laplace(field):
        centre = 2.0 * shifted(field, 0, 0, 0)
        return ((shifted(field, 1, 0, 0) + shifted(field, -1, 0, 0) - centre) * (radial_h * radial_h)
                + (shifted(field, 0, 1, 0) + shifted(field, 0, -1, 0) - centre) * (colat_h * colat_h)
                + (shifted(field, 0, 0, 1) + shifted(field, 0, 0, -1) - centre) * (lon_h * lon_h))

    def cross_of(left_vec, right_vec):
        return jnp.stack([left_vec[1] * right_vec[2] - left_vec[2] * right_vec[1],
                          left_vec[2] * right_vec[0] - left_vec[0] * right_vec[2],
                          left_vec[0] * right_vec[1] - left_vec[1] * right_vec[0]])

    def curl_of(field):
        return jnp.stack([colat_diff(field[2]) - lon_diff(field[1]),
                          lon_diff(field[0]) - radial_diff(field[2]),
                          radial_diff(field[1]) - colat_diff(field[0])])

    density_pad = padded[0]
    flow_pad = padded[1:4]
    magnet_pad = padded[4:7]
    press_pad = padded[7]
    density_c = shifted(density_pad, 0, 0, 0)
    flow_c = shifted(flow_pad, 0, 0, 0)
    magnet_c = shifted(magnet_pad, 0, 0, 0)
    press_c = shifted(press_pad, 0, 0, 0)
    momentum = density_pad[None] * flow_pad
    emf_pad = cross_of(flow_pad, magnet_pad)
    lorentz = cross_of(curl_of(magnet_pad), magnet_c)

    def carried(field):
        return flow_c[0] * radial_diff(field) + flow_c[1] * colat_diff(field) + flow_c[2] * lon_diff(field)

    div_mom = radial_diff(momentum[0]) + colat_diff(momentum[1]) + lon_diff(momentum[2])
    div_flow = radial_diff(flow_pad[0]) + colat_diff(flow_pad[1]) + lon_diff(flow_pad[2])
    press_grad = [radial_diff(press_pad), colat_diff(press_pad), lon_diff(press_pad)]
    new_density = density_c - dt_step * div_mom
    new_flow = jnp.stack([flow_c[comp] + dt_step * (-carried(flow_pad[comp]) + (lorentz[comp] - press_grad[comp]) / density_c + diffusivity * laplace(flow_pad[comp])) for comp in range(3)])
    new_magnet = magnet_c + dt_step * (curl_of(emf_pad) + diffusivity * laplace(magnet_pad))
    new_press = press_c + dt_step * (-carried(press_pad) - GAMMA * press_c * div_flow + diffusivity * laplace(press_pad))
    return new_density, new_flow, new_magnet, new_press


def donor_values(fields, send_row, send_col, send_weight, send_turn):
    tile_first_rows = jnp.arange(N_THETA, dtype=jnp.int32)[:, None, None] * CT
    tile_first_cols = jnp.arange(N_PHI, dtype=jnp.int32)[None, :, None] * CP
    row_index = (tile_first_rows + send_row).reshape(-1)
    col_index = (tile_first_cols + send_col).reshape(-1)
    weight_row = send_weight[:, :, 0, :].reshape(-1)
    weight_col = send_weight[:, :, 1, :].reshape(-1)

    def corner(step_t, step_p):
        return fields[:, :, row_index + step_t, col_index + step_p]

    blended = bilinear(corner(0, 0), corner(0, 1), corner(1, 0), corner(1, 1), weight_row, weight_col)
    return turn_frame(blended, send_turn.reshape(-1))


def advance_patch(fields, border, radius, constants):
    d_theta, d_phi, dt_step, diffusivity = constants
    radial_pad = jnp.pad(fields, ((0, 0), (1, 1), (0, 0), (0, 0)), mode="edge")
    padded = jnp.pad(radial_pad, ((0, 0), (0, 0), (1, 1), (1, 1)))
    upper_side = jnp.transpose(border[:NPH], (1, 2, 0))
    lower_side = jnp.transpose(border[NPH:2 * NPH], (1, 2, 0))
    left_side = jnp.transpose(border[2 * NPH:2 * NPH + NTH], (1, 2, 0))
    right_side = jnp.transpose(border[2 * NPH + NTH:], (1, 2, 0))
    padded = padded.at[:, 1:-1, 0, 1:-1].set(upper_side)
    padded = padded.at[:, 1:-1, -1, 1:-1].set(lower_side)
    padded = padded.at[:, 1:-1, 1:-1, 0].set(left_side)
    padded = padded.at[:, 1:-1, 1:-1, -1].set(right_side)

    def one_block(tile_number):
        first_row = tile_number * CT
        tile_block = lax.dynamic_slice_in_dim(padded, first_row, CT + 2, 2)
        rows_global = first_row + jnp.arange(CT, dtype=jnp.int32)
        sin_theta = jnp.sin(0.25 * math.pi + (rows_global.astype(jnp.float32) + 0.5) * d_theta)
        return advance(tile_block, radius, sin_theta, d_theta, d_phi, dt_step, diffusivity)

    blocks = lax.map(one_block, jnp.arange(N_THETA, dtype=jnp.int32))
    new_density = jnp.moveaxis(blocks[0], 0, -3).reshape(NR, NTH, NPH)
    new_flow = jnp.moveaxis(blocks[1], 0, -3).reshape(3, NR, NTH, NPH)
    new_magnet = jnp.moveaxis(blocks[2], 0, -3).reshape(3, NR, NTH, NPH)
    new_press = jnp.moveaxis(blocks[3], 0, -3).reshape(NR, NTH, NPH)
    return new_density, new_flow, new_magnet, new_press


def reference(density, velocity, magnetic, pressure, send_row, send_col, send_weight, send_turn, send_dest):
    fields = jnp.concatenate([density[:, None], velocity, magnetic, pressure[:, None]], axis=1)
    border_count = 2 * NPH + 2 * NTH
    constants = grid_constants(NTH, NPH)
    radius = R_BASE + (jnp.arange(NR, dtype=jnp.float32) + 0.5) * DR_STEP
    received = []
    for donor_patch in range(2):
        values = donor_values(fields[donor_patch], send_row[donor_patch], send_col[donor_patch], send_weight[donor_patch], send_turn[donor_patch])
        target = send_dest[donor_patch].reshape(-1)
        placed = jnp.zeros((border_count + 1, 8, NR), jnp.float32).at[target].add(jnp.transpose(values, (2, 0, 1)))
        received.append(placed[:border_count])
    results = [advance_patch(fields[which], received[1 - which], radius, constants) for which in range(2)]
    return (jnp.stack([results[0][0], results[1][0]]),
            jnp.stack([results[0][1], results[1][1]]),
            jnp.stack([results[0][2], results[1][2]]),
            jnp.stack([results[0][3], results[1][3]]))
```

```python
import functools
import math

import jax
import jax.numpy as jnp
import numpy as np
from jax import lax
from jax.experimental import pallas as pl
from jax.experimental.pallas import tpu as pltpu
from jax.sharding import PartitionSpec as P

GAMMA = 5.0 / 3.0
R_BASE = 0.6
DR_STEP = 0.65 / 64.0
COURANT = 0.4
DIFFUSE = 0.4
MESH = pl.DeviceIdType.MESH
LANES = 128
HEAD = 8


def grid_constants(total_theta, total_phi):
    d_theta = 0.5 * math.pi / total_theta
    d_phi = 1.5 * math.pi / total_phi
    r_low = R_BASE + 0.5 * DR_STEP
    inv_r = 1.0 / DR_STEP
    inv_t = 1.0 / (r_low * d_theta)
    inv_p = 1.0 / (r_low * math.sin(0.25 * math.pi) * d_phi)
    dt_step = COURANT / (inv_r + inv_t + inv_p)
    diffusivity = DIFFUSE / (dt_step * (inv_r * inv_r + inv_t * inv_t + inv_p * inv_p))
    return (d_theta, d_phi, dt_step, diffusivity)


def split(x):
    hi = x.astype(jnp.bfloat16)
    lo = (x - hi.astype(jnp.float32)).astype(jnp.bfloat16)
    return hi, lo


def dot_nt(a, b):
    return lax.dot_general(a, b, (((1,), (1,)), ((), ())), preferred_element_type=jnp.float32)


def dot_nn(a, b):
    return jnp.dot(a, b, preferred_element_type=jnp.float32)


def exchange_kernel(
    dims, den, vel, mag, prs, srow, scol, swgt, sturn, sdest,
    up_out, down_out, left_out, right_out,
    table, gathered, rows_out, rows_in, cols_out, cols_in, lon_out, lon_in, lat_out, lat_in,
    gather_send, gather_recv, lon_send, lon_recv, lat_send, lat_recv, halo_send, halo_recv,
):
    n_theta, n_phi, levels, tile_rows, tile_cols, slots = dims
    total_phi = tile_cols * n_phi
    total_theta = tile_rows * n_theta
    channels = 8 * levels
    chunks = -(-slots // LANES)
    q = lax.axis_index("patch")
    t = lax.axis_index("theta")
    f = lax.axis_index("phi")
    other = 1 - q

    barrier = pltpu.get_barrier_semaphore()

    def greet(device):
        pl.semaphore_signal(barrier, inc=1, device_id=device, device_id_type=MESH)

    for d in range(1, n_phi):
        greet((q, t, lax.rem(f + d, n_phi)))
    greet((q, lax.rem(t + 1, n_theta), f))
    greet((q, lax.rem(t + n_theta - 1, n_theta), f))
    for d in range(n_theta):
        greet((other, d, f))

    table[...] = jnp.zeros_like(table)
    table[0:1, :slots] = srow[...].astype(jnp.float32)
    table[1:2, :slots] = scol[...].astype(jnp.float32)
    table[2:4, :slots] = swgt[...]
    turn = sturn[...]
    table[4:5, :slots] = jnp.cos(turn)
    table[5:6, :slots] = jnp.sin(turn)
    dest_row = sdest[...].astype(jnp.float32)
    table[6:7, :slots] = dest_row
    columns = table[...].T[:slots]
    row_s = columns[:, 0:1]
    col_s = columns[:, 1:2]
    w_row = columns[:, 2:3]
    w_col = columns[:, 3:4]
    cos_s = columns[:, 4:5]
    sin_s = columns[:, 5:6]

    lane = lax.broadcasted_iota(jnp.int32, (slots, tile_cols), 1).astype(jnp.float32)
    pick = jnp.where(lane == col_s, 1.0 - w_col, 0.0) + jnp.where(lane == col_s + 1.0, w_col, 0.0)
    pick_hi, pick_lo = split(pick)

    def field_row(r):
        return jnp.concatenate(
            [
                den[pl.ds(r, levels, stride=tile_rows), :],
                vel[pl.ds(r, 3 * levels, stride=tile_rows), :],
                mag[pl.ds(r, 3 * levels, stride=tile_rows), :],
                prs[pl.ds(r, levels, stride=tile_rows), :],
            ],
            axis=0,
        )

    value = jnp.zeros((slots, channels), jnp.float32)
    for r in range(tile_rows):
        cells = field_row(r)
        if r == 0:
            rows_out[0] = cells
        if r == tile_rows - 1:
            rows_out[1] = cells
        hi, lo = split(cells)
        part = dot_nt(pick_hi, hi) + (dot_nt(pick_hi, lo) + dot_nt(pick_lo, hi))
        gain = jnp.where(row_s == r, 1.0 - w_row, 0.0) + jnp.where(row_s + 1.0 == r, w_row, 0.0)
        value = value + gain * part
    comp = lax.broadcasted_iota(jnp.int32, (slots, channels), 1) // levels
    first = (comp == 2) | (comp == 5)
    second = (comp == 3) | (comp == 6)
    partner = jnp.where(
        first,
        pltpu.roll(value, channels - levels, axis=1),
        pltpu.roll(value, levels, axis=1),
    )
    keep = jnp.where(first | second, cos_s, 1.0)
    mix = jnp.where(first, sin_s, jnp.where(second, -sin_s, 0.0))
    own = gathered.at[f]
    own[HEAD:HEAD + slots, :] = keep * value + mix * partner
    for c in range(chunks):
        own[c:c + 1, :] = table[6:7, c * LANES:(c + 1) * LANES]

    pl.semaphore_wait(barrier, n_phi - 1 + 2 + n_theta)

    def gather_copy(d):
        return pltpu.make_async_remote_copy(
            src_ref=gathered.at[f],
            dst_ref=gathered.at[f],
            send_sem=gather_send.at[d - 1],
            recv_sem=gather_recv.at[d - 1],
            device_id=(q, t, lax.rem(f + d, n_phi)),
            device_id_type=MESH,
        )

    for d in range(1, n_phi):
        gather_copy(d).start()

    def row_copy(way):
        return pltpu.make_async_remote_copy(
            src_ref=rows_out.at[way],
            dst_ref=rows_in.at[way],
            send_sem=halo_send.at[way],
            recv_sem=halo_recv.at[way],
            device_id=(q, lax.rem(t + (1 if way else n_theta - 1), n_theta), f),
            device_id_type=MESH,
        )

    def col_copy(way):
        return pltpu.make_async_remote_copy(
            src_ref=cols_out.at[way],
            dst_ref=cols_in.at[way],
            send_sem=halo_send.at[2 + way],
            recv_sem=halo_recv.at[2 + way],
            device_id=(q, t, lax.rem(f + (1 if way else n_phi - 1), n_phi)),
            device_id_type=MESH,
        )

    @pl.when(t > 0)
    def _():
        row_copy(0).start()

    @pl.when(t < n_theta - 1)
    def _():
        row_copy(1).start()

    lane2 = lax.broadcasted_iota(jnp.int32, (tile_rows, channels), 1)
    low = jnp.zeros((tile_rows, channels), jnp.float32)
    high = jnp.zeros((tile_rows, channels), jnp.float32)
    for c in range(8):
        ref, base = ((den, 0), (vel, 0), (vel, 1), (vel, 2), (mag, 0), (mag, 1), (mag, 2), (prs, 0))[c]
        for k in range(levels):
            cells = ref[(base * levels + k) * tile_rows:(base * levels + k + 1) * tile_rows, :]
            hit = lane2 == c * levels + k
            low = jnp.where(hit, cells[:, 0:1], low)
            high = jnp.where(hit, cells[:, tile_cols - 1:tile_cols], high)
    cols_out[0] = low
    cols_out[1] = high

    def ids_of(count):
        return lax.broadcasted_iota(jnp.int32, (count, LANES), 0)

    ids_top = ids_of(tile_cols) + f * tile_cols
    lat_base = 2 * total_phi + jnp.where(f == 0, 0, total_theta)
    ids = jnp.concatenate(
        [ids_top, ids_top + total_phi, ids_of(total_theta) + lat_base], axis=0
    ).astype(jnp.float32)

    def place(slot_ref):
        total = None
        for c in range(chunks):
            size = min(LANES, slots - c * LANES)
            hits = jnp.where(ids == slot_ref[c:c + 1, :], 1.0, 0.0).astype(jnp.bfloat16)
            hi, lo = split(slot_ref[HEAD + c * LANES:HEAD + c * LANES + size, :])
            hits = hits[:, :size]
            term = dot_nn(hits, hi) + dot_nn(hits, lo)
            total = term if total is None else total + term
        return total

    @pl.when(f > 0)
    def _():
        col_copy(0).start()

    @pl.when(f < n_phi - 1)
    def _():
        col_copy(1).start()

    placed = place(gathered.at[f])
    for d in range(1, n_phi):
        source = lax.rem(f + n_phi - d, n_phi)
        pltpu.make_async_remote_copy(
            src_ref=gathered.at[source],
            dst_ref=gathered.at[source],
            send_sem=gather_send.at[d - 1],
            recv_sem=gather_recv.at[d - 1],
            device_id=(q, t, source),
            device_id_type=MESH,
        ).wait_recv()
        placed = placed + place(gathered.at[source])
    lon_out[0] = placed[:tile_cols]
    lon_out[1] = placed[tile_cols:2 * tile_cols]
    lat_out[...] = placed[2 * tile_cols:]

    def lon_copy(side):
        return pltpu.make_async_remote_copy(
            src_ref=lon_out.at[side],
            dst_ref=lon_in.at[t],
            send_sem=lon_send.at[side],
            recv_sem=lon_recv.at[t],
            device_id=(other, (n_theta - 1) * side, f),
            device_id_type=MESH,
        )

    def lat_copy(d):
        return pltpu.make_async_remote_copy(
            src_ref=lat_out.at[pl.ds(d * tile_rows, tile_rows)],
            dst_ref=lat_in.at[t],
            send_sem=lat_send.at[d],
            recv_sem=lat_recv.at[t],
            device_id=(other, d, f),
            device_id_type=MESH,
        )

    lon_copy(0).start()
    lon_copy(1).start()

    at_side = (f == 0) | (f == n_phi - 1)
    at_end = (t == 0) | (t == n_theta - 1)

    @pl.when(at_side)
    def _():
        for d in range(n_theta):
            lat_copy(d).start()

    @pl.when(t > 0)
    def _():
        row_copy(1).wait_recv()
        up_out[...] = rows_in[1]

    @pl.when(t < n_theta - 1)
    def _():
        row_copy(0).wait_recv()
        down_out[...] = rows_in[0]

    @pl.when(f > 0)
    def _():
        col_copy(1).wait_recv()
        left_out[...] = cols_in[1]

    @pl.when(f < n_phi - 1)
    def _():
        col_copy(0).wait_recv()
        right_out[...] = cols_in[0]

    @pl.when(at_end)
    def _():
        for s in range(n_theta):
            pltpu.make_async_remote_copy(
                src_ref=lon_in.at[s],
                dst_ref=lon_in.at[s],
                send_sem=lon_send.at[0],
                recv_sem=lon_recv.at[s],
                device_id=(other, s, f),
                device_id_type=MESH,
            ).wait_recv()
        total = lon_in[0]
        for s in range(1, n_theta):
            total = total + lon_in[s]
        total = total.T

        @pl.when(t == 0)
        def _():
            up_out[...] = total

        @pl.when(t == n_theta - 1)
        def _():
            down_out[...] = total

    @pl.when(at_side)
    def _():
        for s in range(n_theta):
            pltpu.make_async_remote_copy(
                src_ref=lat_in.at[s],
                dst_ref=lat_in.at[s],
                send_sem=lat_send.at[0],
                recv_sem=lat_recv.at[s],
                device_id=(other, s, f),
                device_id_type=MESH,
            ).wait_recv()
        total = lat_in[0]
        for s in range(1, n_theta):
            total = total + lat_in[s]

        @pl.when(f == 0)
        def _():
            left_out[...] = total

        @pl.when(f == n_phi - 1)
        def _():
            right_out[...] = total

    for d in range(1, n_phi):
        gather_copy(d).wait_send()
    lon_copy(0).wait_send()
    lon_copy(1).wait_send()

    @pl.when(at_side)
    def _():
        for d in range(n_theta):
            lat_copy(d).wait_send()

    @pl.when(t > 0)
    def _():
        row_copy(0).wait_send()

    @pl.when(t < n_theta - 1)
    def _():
        row_copy(1).wait_send()

    @pl.when(f > 0)
    def _():
        col_copy(0).wait_send()

    @pl.when(f < n_phi - 1)
    def _():
        col_copy(1).wait_send()


def stencil_kernel(
    dims, den, vel, mag, prs, up, down, left, right, metric, inv_radius,
    new_den, new_vel, new_mag, new_prs,
):
    n_theta, n_phi, levels, rows, cols, _ = dims
    d_theta, _, dt_step, diffusivity = grid_constants(rows * n_theta, cols * n_phi)
    g_r = 1.0 / DR_STEP
    first_row = pl.multiple_of(lax.axis_index("theta") * rows, rows)
    lon_row = metric[pl.ds(first_row, rows), :]
    row_id = lax.broadcasted_iota(jnp.int32, (rows, cols), 0)
    col_id = lax.broadcasted_iota(jnp.int32, (rows, cols), 1)
    at_up = row_id == 0
    at_down = row_id == rows - 1
    at_left = col_id == 0
    at_right = col_id == cols - 1
    sources = ((den, 0), (vel, 0), (vel, 1), (vel, 2), (mag, 0), (mag, 1), (mag, 2), (prs, 0))
    channels = 8 * levels

    def level(k, carry):
        inv_rk = inv_radius[k]
        g_t = inv_rk * (1.0 / d_theta)
        g_p = lon_row * inv_rk
        half_r = 0.5 * g_r
        half_t = 0.5 * g_t
        half_p = 0.5 * g_p
        below = jnp.maximum(k - 1, 0)
        above = jnp.minimum(k + 1, levels - 1)

        def load(c, kk):
            ref, base = sources[c]
            return ref[pl.ds(pl.multiple_of((base * levels + kk) * rows, rows), rows), :]

        mid = [load(c, k) for c in range(8)]
        r_lo = [load(c, below) for c in range(8)]
        r_hi = [load(c, above) for c in range(8)]
        left_all = left[...]
        right_all = right[...]
        t_lo, t_hi, p_lo, p_hi = [], [], [], []
        for c in range(8):
            u = mid[c]
            ck = c * levels + k
            t_lo.append(jnp.where(at_up, up[pl.ds(ck, 1), :], pltpu.roll(u, 1, axis=0)))
            t_hi.append(jnp.where(at_down, down[pl.ds(ck, 1), :], pltpu.roll(u, rows - 1, axis=0)))
            p_lo.append(
                jnp.where(at_left, pltpu.roll(left_all, channels - ck, axis=1), pltpu.roll(u, 1, axis=1))
            )
            p_hi.append(
                jnp.where(
                    at_right,
                    pltpu.roll(right_all, channels - 1 - ck, axis=1),
                    pltpu.roll(u, cols - 1, axis=1),
                )
            )

        def dr(c):
            return (r_hi[c] - r_lo[c]) * half_r

        def dth(c):
            return (t_hi[c] - t_lo[c]) * half_t

        def dp(c):
            return (p_hi[c] - p_lo[c]) * half_p

        rr = g_r * g_r
        tt = g_t * g_t
        pp = g_p * g_p

        def laplace(c):
            centre = 2.0 * mid[c]
            return (
                (r_hi[c] + r_lo[c] - centre) * rr
                + (t_hi[c] + t_lo[c] - centre) * tt
                + (p_hi[c] + p_lo[c] - centre) * pp
            )

        v_r, v_t, v_p = mid[1], mid[2], mid[3]
        b_r, b_t, b_p = mid[4], mid[5], mid[6]
        rho, press = mid[0], mid[7]
        div_mom = (
            (r_hi[0] * r_hi[1] - r_lo[0] * r_lo[1]) * half_r
            + (t_hi[0] * t_hi[2] - t_lo[0] * t_lo[2]) * half_t
            + (p_hi[0] * p_hi[3] - p_lo[0] * p_lo[3]) * half_p
        )

        def put(ref, base, x):
            ref[pl.ds(pl.multiple_of((base * levels + k) * rows, rows), rows), :] = x

        put(new_den, 0, rho - dt_step * div_mom)

        grads = [(dr(c), dth(c), dp(c)) for c in range(1, 4)]
        inv_rho = 1.0 / rho
        j_r = dth(6) - dp(5)
        j_t = dp(4) - dr(6)
        j_p = dr(5) - dth(4)
        lorentz = (j_t * b_p - j_p * b_t, j_p * b_r - j_r * b_p, j_r * b_t - j_t * b_r)
        p_grad = (dr(7), dth(7), dp(7))
        for i in range(3):
            g = grads[i]
            carried = v_r * g[0] + v_t * g[1] + v_p * g[2]
            put(
                new_vel, i,
                mid[1 + i]
                + dt_step
                * ((lorentz[i] - p_grad[i]) * inv_rho - carried + diffusivity * laplace(1 + i)),
            )

        def emf(s, i):
            a, b = ((2, 3), (3, 1), (1, 2))[i]
            return s[a] * s[b + 3] - s[b] * s[a + 3]

        def diff(lo, hi, i):
            return emf(hi, i) - emf(lo, i)

        curl = (
            diff(t_lo, t_hi, 2) * half_t - diff(p_lo, p_hi, 1) * half_p,
            diff(p_lo, p_hi, 0) * half_p - diff(r_lo, r_hi, 2) * half_r,
            diff(r_lo, r_hi, 1) * half_r - diff(t_lo, t_hi, 0) * half_t,
        )
        for i in range(3):
            put(new_mag, i, mid[4 + i] + dt_step * (curl[i] + diffusivity * laplace(4 + i)))
        div_flow = grads[0][0] + grads[1][1] + grads[2][2]
        carried = v_r * p_grad[0] + v_t * p_grad[1] + v_p * p_grad[2]
        put(
            new_prs, 0,
            press + dt_step * (diffusivity * laplace(7) - carried - GAMMA * press * div_flow),
        )
        return carry

    lax.fori_loop(0, levels, level, 0)


def body(
    n_theta, n_phi,
    density, velocity, magnetic, pressure, send_row, send_col, send_weight, send_turn, send_dest,
):
    levels, tile_rows, tile_cols = density.shape[1:]
    slots = send_row.shape[-1]
    dims = (n_theta, n_phi, levels, tile_rows, tile_cols, slots)
    channels = 8 * levels
    chunks = -(-slots // LANES)
    total_theta = n_theta * tile_rows
    _, d_phi, _, _ = grid_constants(total_theta, n_phi * tile_cols)
    d_theta = 0.5 * math.pi / total_theta
    fields = [x.reshape(-1, tile_cols) for x in (density, velocity, magnetic, pressure)]
    vmem = pl.BlockSpec(memory_space=pltpu.VMEM)
    f32 = jnp.float32
    dma = pltpu.SemaphoreType.DMA
    tile_row = jax.ShapeDtypeStruct((channels, tile_cols), f32)
    tile_col = jax.ShapeDtypeStruct((tile_rows, channels), f32)
    up, down, left, right = pl.pallas_call(
        functools.partial(exchange_kernel, dims),
        out_shape=(tile_row, tile_row, tile_col, tile_col),
        in_specs=[vmem] * 9,
        out_specs=(vmem,) * 4,
        scratch_shapes=[
            pltpu.VMEM((LANES, chunks * LANES), f32),
            pltpu.VMEM((n_phi, HEAD + slots, channels), f32),
            pltpu.VMEM((2, channels, tile_cols), f32),
            pltpu.VMEM((2, channels, tile_cols), f32),
            pltpu.VMEM((2, tile_rows, channels), f32),
            pltpu.VMEM((2, tile_rows, channels), f32),
            pltpu.VMEM((2, tile_cols, channels), f32),
            pltpu.VMEM((n_theta, tile_cols, channels), f32),
            pltpu.VMEM((total_theta, channels), f32),
            pltpu.VMEM((n_theta, tile_rows, channels), f32),
            dma((n_phi - 1,)),
            dma((n_phi - 1,)),
            dma((2,)),
            dma((n_theta,)),
            dma((n_theta,)),
            dma((n_theta,)),
            dma((4,)),
            dma((4,)),
        ],
        compiler_params=pltpu.CompilerParams(collective_id=0, has_side_effects=True),
        name="exchange",
    )(
        *fields,
        send_row.reshape(1, slots),
        send_col.reshape(1, slots),
        send_weight.reshape(2, slots),
        send_turn.reshape(1, slots),
        send_dest.reshape(1, slots),
    )
    thetas = 0.25 * math.pi + (np.arange(total_theta) + 0.5) * d_theta
    metric = np.broadcast_to(
        (1.0 / (np.sin(thetas) * d_phi))[:, None], (total_theta, tile_cols)
    ).astype(np.float32)
    radius = R_BASE + (np.arange(levels) + 0.5) * DR_STEP
    outs = pl.pallas_call(
        functools.partial(stencil_kernel, dims),
        out_shape=tuple(jax.ShapeDtypeStruct(x.shape, f32) for x in fields),
        in_specs=[vmem] * 9 + [pl.BlockSpec(memory_space=pltpu.SMEM)],
        out_specs=(vmem,) * 4,
        name="stencil",
    )(*fields, up, down, left, right, jnp.asarray(metric), jnp.asarray((1.0 / radius).astype(np.float32)))
    return tuple(
        x.reshape(like.shape) for x, like in zip(outs, (density, velocity, magnetic, pressure))
    )


def solution(mesh):
    scalar = P("patch", None, "theta", "phi")
    vector = P("patch", None, None, "theta", "phi")
    slot = P("patch", "theta", "phi", None)
    return jax.shard_map(
        functools.partial(body, mesh.shape["theta"], mesh.shape["phi"]),
        mesh=mesh,
        in_specs=(
            scalar, vector, vector, scalar, slot, slot,
            P("patch", "theta", "phi", None, None), slot, slot,
        ),
        out_specs=(scalar, vector, vector, scalar),
        check_vma=False,
    )
```

```python
import functools
import math

import jax
import jax.numpy as jnp
import numpy as np
from jax import lax
from jax.experimental import pallas as pl
from jax.experimental.pallas import tpu as pltpu
from jax.sharding import PartitionSpec as P

GAMMA = 5.0 / 3.0
R_BASE = 0.6
DR_STEP = 0.65 / 64.0
COURANT = 0.4
DIFFUSE = 0.4
MESH = pl.DeviceIdType.MESH
LANES = 128
HEAD = 8


def grid_constants(total_theta, total_phi):
    d_theta = 0.5 * math.pi / total_theta
    d_phi = 1.5 * math.pi / total_phi
    r_low = R_BASE + 0.5 * DR_STEP
    inv_r = 1.0 / DR_STEP
    inv_t = 1.0 / (r_low * d_theta)
    inv_p = 1.0 / (r_low * math.sin(0.25 * math.pi) * d_phi)
    dt_step = COURANT / (inv_r + inv_t + inv_p)
    diffusivity = DIFFUSE / (dt_step * (inv_r * inv_r + inv_t * inv_t + inv_p * inv_p))
    return (d_theta, d_phi, dt_step, diffusivity)


def split(x):
    hi = x.astype(jnp.bfloat16)
    lo = (x - hi.astype(jnp.float32)).astype(jnp.bfloat16)
    return hi, lo


def dot_nt(a, b):
    return lax.dot_general(a, b, (((1,), (1,)), ((), ())), preferred_element_type=jnp.float32)


def dot_nn(a, b):
    return jnp.dot(a, b, preferred_element_type=jnp.float32)


def exchange_kernel(
    dims, den, vel, mag, prs, srow, scol, swgt, sturn, sdest,
    up_out, down_out, left_out, right_out,
    table, gathered, rows_out, rows_in, cols_out, cols_in, lon_out, lon_in, lat_out, lat_in,
    gather_send, gather_recv, lon_send, lon_recv, lat_send, lat_recv, halo_send, halo_recv,
):
    n_theta, n_phi, levels, tile_rows, tile_cols, slots = dims
    total_phi = tile_cols * n_phi
    total_theta = tile_rows * n_theta
    channels = 8 * levels
    chunks = -(-slots // LANES)
    q = lax.axis_index("patch")
    t = lax.axis_index("theta")
    f = lax.axis_index("phi")
    other = 1 - q

    barrier = pltpu.get_barrier_semaphore()

    def greet(device):
        pl.semaphore_signal(barrier, inc=1, device_id=device, device_id_type=MESH)

    for d in range(1, n_phi):
        greet((q, t, lax.rem(f + d, n_phi)))
    greet((q, lax.rem(t + 1, n_theta), f))
    greet((q, lax.rem(t + n_theta - 1, n_theta), f))
    for d in range(n_theta):
        greet((other, d, f))

    table[...] = jnp.zeros_like(table)
    table[0:1, :slots] = srow[...].astype(jnp.float32)
    table[1:2, :slots] = scol[...].astype(jnp.float32)
    table[2:4, :slots] = swgt[...]
    turn = sturn[...]
    table[4:5, :slots] = jnp.cos(turn)
    table[5:6, :slots] = jnp.sin(turn)
    table[6:7, :slots] = sdest[...].astype(jnp.float32)
    columns = table[...].T[:slots]
    row_s = columns[:, 0:1]
    col_s = columns[:, 1:2]
    w_row = columns[:, 2:3]
    w_col = columns[:, 3:4]
    half = slots // 2
    width = channels // 2
    fold_lane = lax.broadcasted_iota(jnp.int32, (half, channels), 1)
    lower = fold_lane < width

    def fold(x):
        return jnp.where(lower, x[:half], x[half:])

    lane = lax.broadcasted_iota(jnp.int32, (slots, tile_cols), 1).astype(jnp.float32)
    pick = jnp.where(lane == col_s, 1.0 - w_col, 0.0) + jnp.where(lane == col_s + 1.0, w_col, 0.0)
    pick_hi, pick_lo = split(pick)
    row_f = fold(row_s)
    w_row_f = fold(w_row)
    cos_f = fold(columns[:, 4:5])
    sin_f = fold(columns[:, 5:6])
    head = table[0:8, :]
    head_lane = lax.broadcasted_iota(jnp.int32, (1, LANES), 1)
    own_dest = (
        head[6:7, :LANES],
        pltpu.roll(head, chunks * LANES - half, axis=1)[6:7, :LANES],
    )
    for c in range(2):
        gathered[0, f, c:c + 1, :] = jnp.where(head_lane < half, own_dest[c], -1.0)

    def field_row(h, r):
        if h == 0:
            parts = [
                den[pl.ds(r, levels, stride=tile_rows), :],
                vel[pl.ds(r, 3 * levels, stride=tile_rows), :],
            ]
        else:
            parts = [
                mag[pl.ds(r, 3 * levels, stride=tile_rows), :],
                prs[pl.ds(r, levels, stride=tile_rows), :],
            ]
        return jnp.concatenate(parts, axis=0)

    def donors(h):
        value = jnp.zeros((half, channels), jnp.float32)
        for r in range(tile_rows):
            cells = field_row(h, r)
            if r == 0:
                rows_out[0, h * width:(h + 1) * width] = cells
            if r == tile_rows - 1:
                rows_out[1, h * width:(h + 1) * width] = cells
            hi, lo = split(jnp.concatenate([cells, cells], axis=0))
            part = dot_nt(pick_hi, hi) + (dot_nt(pick_hi, lo) + dot_nt(pick_lo, hi))
            gain = jnp.where(row_f == r, 1.0 - w_row_f, 0.0) + jnp.where(row_f + 1.0 == r, w_row_f, 0.0)
            value = value + gain * fold(part)
        comp = lax.rem(fold_lane, width) // levels + 4 * h
        first = (comp == 2) | (comp == 5)
        second = (comp == 3) | (comp == 6)
        partner = jnp.where(
            first,
            pltpu.roll(value, channels - levels, axis=1),
            pltpu.roll(value, levels, axis=1),
        )
        keep = jnp.where(first | second, cos_f, 1.0)
        mix = jnp.where(first, sin_f, jnp.where(second, -sin_f, 0.0))
        gathered[h, f, HEAD:HEAD + half, :] = keep * value + mix * partner

    def donor_ref(h, source):
        if h == 0:
            return gathered.at[0, source]
        return gathered.at[1, source, pl.ds(HEAD, half)]

    def gather_copy(h, d, source=None):
        at = f if source is None else source
        return pltpu.make_async_remote_copy(
            src_ref=donor_ref(h, at),
            dst_ref=donor_ref(h, at),
            send_sem=gather_send.at[h * (n_phi - 1) + d - 1],
            recv_sem=gather_recv.at[h * (n_phi - 1) + d - 1],
            device_id=(q, t, lax.rem(f + d, n_phi) if source is None else source),
            device_id_type=MESH,
        )

    donors(0)
    pl.semaphore_wait(barrier, n_phi - 1 + 2 + n_theta)
    for d in range(1, n_phi):
        gather_copy(0, d).start()
    donors(1)
    for d in range(1, n_phi):
        gather_copy(1, d).start()

    def row_copy(way):
        return pltpu.make_async_remote_copy(
            src_ref=rows_out.at[way],
            dst_ref=rows_in.at[way],
            send_sem=halo_send.at[way],
            recv_sem=halo_recv.at[way],
            device_id=(q, lax.rem(t + (1 if way else n_theta - 1), n_theta), f),
            device_id_type=MESH,
        )

    def col_copy(way):
        return pltpu.make_async_remote_copy(
            src_ref=cols_out.at[way],
            dst_ref=cols_in.at[way],
            send_sem=halo_send.at[2 + way],
            recv_sem=halo_recv.at[2 + way],
            device_id=(q, t, lax.rem(f + (1 if way else n_phi - 1), n_phi)),
            device_id_type=MESH,
        )

    @pl.when(t > 0)
    def _():
        row_copy(0).start()

    @pl.when(t < n_theta - 1)
    def _():
        row_copy(1).start()

    lane2 = lax.broadcasted_iota(jnp.int32, (tile_rows, channels), 1)
    low = jnp.zeros((tile_rows, channels), jnp.float32)
    high = jnp.zeros((tile_rows, channels), jnp.float32)
    for c in range(8):
        ref, base = ((den, 0), (vel, 0), (vel, 1), (vel, 2), (mag, 0), (mag, 1), (mag, 2), (prs, 0))[c]
        for k in range(levels):
            cells = ref[(base * levels + k) * tile_rows:(base * levels + k + 1) * tile_rows, :]
            hit = lane2 == c * levels + k
            low = jnp.where(hit, cells[:, 0:1], low)
            high = jnp.where(hit, cells[:, tile_cols - 1:tile_cols], high)
    cols_out[0] = low
    cols_out[1] = high

    def ids_of(count):
        return lax.broadcasted_iota(jnp.int32, (count, LANES), 0)

    ids_top = ids_of(tile_cols) + f * tile_cols
    lat_base = 2 * total_phi + jnp.where(f == 0, 0, total_theta)
    ids = jnp.concatenate(
        [ids_top, ids_top + total_phi, ids_of(total_theta) + lat_base], axis=0
    ).astype(jnp.float32)

    def place(h, source):
        folded = gathered[h, source, HEAD:HEAD + half, :]
        total = None
        for c in range(2):
            hits = jnp.where(ids == gathered[0, source, c:c + 1, :], 1.0, 0.0).astype(jnp.bfloat16)[:, :half]
            hi, lo = split(folded if c == 0 else pltpu.roll(folded, width, axis=1))
            term = dot_nn(hits, hi) + dot_nn(hits, lo)
            total = term if total is None else total + term
        return total

    @pl.when(f > 0)
    def _():
        col_copy(0).start()

    @pl.when(f < n_phi - 1)
    def _():
        col_copy(1).start()

    short = tile_cols // 2
    lon_lower = lax.broadcasted_iota(jnp.int32, (short, channels), 1) < width

    def lon_copy(h, side):
        return pltpu.make_async_remote_copy(
            src_ref=lon_out.at[h, side],
            dst_ref=lon_in.at[h, t],
            send_sem=lon_send.at[2 * h + side],
            recv_sem=lon_recv.at[h * n_theta + t],
            device_id=(other, (n_theta - 1) * side, f),
            device_id_type=MESH,
        )

    lat_parts = []
    for h in range(2):
        placed = place(h, f)
        for d in range(1, n_phi):
            source = lax.rem(f + n_phi - d, n_phi)
            gather_copy(h, d, source).wait_recv()
            placed = placed + place(h, source)
        for side in range(2):
            base = side * tile_cols
            lon_out[h, side] = jnp.where(
                lon_lower,
                placed[base:base + short],
                pltpu.roll(placed[base + short:base + tile_cols], width, axis=1),
            )
        lat_parts.append(placed[2 * tile_cols:])
        lon_copy(h, 0).start()
        lon_copy(h, 1).start()
    lat_lower = lax.broadcasted_iota(jnp.int32, (total_theta, channels), 1) < width
    lat_out[...] = jnp.where(lat_lower, lat_parts[0], pltpu.roll(lat_parts[1], width, axis=1))

    def lat_copy(d):
        return pltpu.make_async_remote_copy(
            src_ref=lat_out.at[pl.ds(d * tile_rows, tile_rows)],
            dst_ref=lat_in.at[t],
            send_sem=lat_send.at[d],
            recv_sem=lat_recv.at[t],
            device_id=(other, d, f),
            device_id_type=MESH,
        )

    at_side = (f == 0) | (f == n_phi - 1)
    at_end = (t == 0) | (t == n_theta - 1)

    @pl.when(at_side)
    def _():
        for d in range(n_theta):
            lat_copy(d).start()

    @pl.when(t > 0)
    def _():
        row_copy(1).wait_recv()
        up_out[...] = rows_in[1]

    @pl.when(t < n_theta - 1)
    def _():
        row_copy(0).wait_recv()
        down_out[...] = rows_in[0]

    @pl.when(f > 0)
    def _():
        col_copy(1).wait_recv()
        left_out[...] = cols_in[1]

    @pl.when(f < n_phi - 1)
    def _():
        col_copy(0).wait_recv()
        right_out[...] = cols_in[0]

    @pl.when(at_end)
    def _():
        sums = []
        for h in range(2):
            total = None
            for s in range(n_theta):
                pltpu.make_async_remote_copy(
                    src_ref=lon_in.at[h, s],
                    dst_ref=lon_in.at[h, s],
                    send_sem=lon_send.at[0],
                    recv_sem=lon_recv.at[h * n_theta + s],
                    device_id=(other, s, f),
                    device_id_type=MESH,
                ).wait_recv()
                total = lon_in[h, s] if total is None else total + lon_in[h, s]
            sums.append(total)
        total = jnp.concatenate(
            [
                jnp.where(lon_lower, sums[0], pltpu.roll(sums[1], width, axis=1)),
                jnp.where(lon_lower, pltpu.roll(sums[0], width, axis=1), sums[1]),
            ],
            axis=0,
        )
        total = total.T

        @pl.when(t == 0)
        def _():
            up_out[...] = total

        @pl.when(t == n_theta - 1)
        def _():
            down_out[...] = total

    @pl.when(at_side)
    def _():
        for s in range(n_theta):
            pltpu.make_async_remote_copy(
                src_ref=lat_in.at[s],
                dst_ref=lat_in.at[s],
                send_sem=lat_send.at[0],
                recv_sem=lat_recv.at[s],
                device_id=(other, s, f),
                device_id_type=MESH,
            ).wait_recv()
        total = lat_in[0]
        for s in range(1, n_theta):
            total = total + lat_in[s]

        @pl.when(f == 0)
        def _():
            left_out[...] = total

        @pl.when(f == n_phi - 1)
        def _():
            right_out[...] = total

    for h in range(2):
        for d in range(1, n_phi):
            gather_copy(h, d).wait_send()
        lon_copy(h, 0).wait_send()
        lon_copy(h, 1).wait_send()

    @pl.when(at_side)
    def _():
        for d in range(n_theta):
            lat_copy(d).wait_send()

    @pl.when(t > 0)
    def _():
        row_copy(0).wait_send()

    @pl.when(t < n_theta - 1)
    def _():
        row_copy(1).wait_send()

    @pl.when(f > 0)
    def _():
        col_copy(0).wait_send()

    @pl.when(f < n_phi - 1)
    def _():
        col_copy(1).wait_send()


def stencil_kernel(
    dims, den, vel, mag, prs, up, down, left, right, metric, inv_radius,
    new_den, new_vel, new_mag, new_prs,
):
    n_theta, n_phi, levels, rows, cols, _ = dims
    d_theta, _, dt_step, diffusivity = grid_constants(rows * n_theta, cols * n_phi)
    g_r = 1.0 / DR_STEP
    first_row = pl.multiple_of(lax.axis_index("theta") * rows, rows)
    lon_row = metric[pl.ds(first_row, rows), :]
    row_id = lax.broadcasted_iota(jnp.int32, (rows, cols), 0)
    col_id = lax.broadcasted_iota(jnp.int32, (rows, cols), 1)
    at_up = row_id == 0
    at_down = row_id == rows - 1
    at_left = col_id == 0
    at_right = col_id == cols - 1
    sources = ((den, 0), (vel, 0), (vel, 1), (vel, 2), (mag, 0), (mag, 1), (mag, 2), (prs, 0))
    channels = 8 * levels

    def level(k, carry):
        inv_rk = inv_radius[k]
        g_t = inv_rk * (1.0 / d_theta)
        g_p = lon_row * inv_rk
        half_r = 0.5 * g_r
        half_t = 0.5 * g_t
        half_p = 0.5 * g_p
        below = jnp.maximum(k - 1, 0)
        above = jnp.minimum(k + 1, levels - 1)

        def load(c, kk):
            ref, base = sources[c]
            return ref[pl.ds(pl.multiple_of((base * levels + kk) * rows, rows), rows), :]

        mid = [load(c, k) for c in range(8)]
        r_lo = [load(c, below) for c in range(8)]
        r_hi = [load(c, above) for c in range(8)]
        left_all = left[...]
        right_all = right[...]
        t_lo, t_hi, p_lo, p_hi = [], [], [], []
        for c in range(8):
            u = mid[c]
            ck = c * levels + k
            t_lo.append(jnp.where(at_up, up[pl.ds(ck, 1), :], pltpu.roll(u, 1, axis=0)))
            t_hi.append(jnp.where(at_down, down[pl.ds(ck, 1), :], pltpu.roll(u, rows - 1, axis=0)))
            p_lo.append(
                jnp.where(at_left, pltpu.roll(left_all, channels - ck, axis=1), pltpu.roll(u, 1, axis=1))
            )
            p_hi.append(
                jnp.where(
                    at_right,
                    pltpu.roll(right_all, channels - 1 - ck, axis=1),
                    pltpu.roll(u, cols - 1, axis=1),
                )
            )

        def dr(c):
            return (r_hi[c] - r_lo[c]) * half_r

        def dth(c):
            return (t_hi[c] - t_lo[c]) * half_t

        def dp(c):
            return (p_hi[c] - p_lo[c]) * half_p

        rr = g_r * g_r
        tt = g_t * g_t
        pp = g_p * g_p

        def laplace(c):
            centre = 2.0 * mid[c]
            return (
                (r_hi[c] + r_lo[c] - centre) * rr
                + (t_hi[c] + t_lo[c] - centre) * tt
                + (p_hi[c] + p_lo[c] - centre) * pp
            )

        v_r, v_t, v_p = mid[1], mid[2], mid[3]
        b_r, b_t, b_p = mid[4], mid[5], mid[6]
        rho, press = mid[0], mid[7]
        div_mom = (
            (r_hi[0] * r_hi[1] - r_lo[0] * r_lo[1]) * half_r
            + (t_hi[0] * t_hi[2] - t_lo[0] * t_lo[2]) * half_t
            + (p_hi[0] * p_hi[3] - p_lo[0] * p_lo[3]) * half_p
        )

        def put(ref, base, x):
            ref[pl.ds(pl.multiple_of((base * levels + k) * rows, rows), rows), :] = x

        put(new_den, 0, rho - dt_step * div_mom)

        grads = [(dr(c), dth(c), dp(c)) for c in range(1, 4)]
        inv_rho = 1.0 / rho
        j_r = dth(6) - dp(5)
        j_t = dp(4) - dr(6)
        j_p = dr(5) - dth(4)
        lorentz = (j_t * b_p - j_p * b_t, j_p * b_r - j_r * b_p, j_r * b_t - j_t * b_r)
        p_grad = (dr(7), dth(7), dp(7))
        for i in range(3):
            g = grads[i]
            carried = v_r * g[0] + v_t * g[1] + v_p * g[2]
            put(
                new_vel, i,
                mid[1 + i]
                + dt_step
                * ((lorentz[i] - p_grad[i]) * inv_rho - carried + diffusivity * laplace(1 + i)),
            )

        def emf(s, i):
            a, b = ((2, 3), (3, 1), (1, 2))[i]
            return s[a] * s[b + 3] - s[b] * s[a + 3]

        def diff(lo, hi, i):
            return emf(hi, i) - emf(lo, i)

        curl = (
            diff(t_lo, t_hi, 2) * half_t - diff(p_lo, p_hi, 1) * half_p,
            diff(p_lo, p_hi, 0) * half_p - diff(r_lo, r_hi, 2) * half_r,
            diff(r_lo, r_hi, 1) * half_r - diff(t_lo, t_hi, 0) * half_t,
        )
        for i in range(3):
            put(new_mag, i, mid[4 + i] + dt_step * (curl[i] + diffusivity * laplace(4 + i)))
        div_flow = grads[0][0] + grads[1][1] + grads[2][2]
        carried = v_r * p_grad[0] + v_t * p_grad[1] + v_p * p_grad[2]
        put(
            new_prs, 0,
            press + dt_step * (diffusivity * laplace(7) - carried - GAMMA * press * div_flow),
        )
        return carry

    lax.fori_loop(0, levels, level, 0)


def body(
    n_theta, n_phi,
    density, velocity, magnetic, pressure, send_row, send_col, send_weight, send_turn, send_dest,
):
    levels, tile_rows, tile_cols = density.shape[1:]
    slots = send_row.shape[-1]
    dims = (n_theta, n_phi, levels, tile_rows, tile_cols, slots)
    channels = 8 * levels
    chunks = -(-slots // LANES)
    total_theta = n_theta * tile_rows
    _, d_phi, _, _ = grid_constants(total_theta, n_phi * tile_cols)
    d_theta = 0.5 * math.pi / total_theta
    fields = [x.reshape(-1, tile_cols) for x in (density, velocity, magnetic, pressure)]
    vmem = pl.BlockSpec(memory_space=pltpu.VMEM)
    f32 = jnp.float32
    dma = pltpu.SemaphoreType.DMA
    tile_row = jax.ShapeDtypeStruct((channels, tile_cols), f32)
    tile_col = jax.ShapeDtypeStruct((tile_rows, channels), f32)
    up, down, left, right = pl.pallas_call(
        functools.partial(exchange_kernel, dims),
        out_shape=(tile_row, tile_row, tile_col, tile_col),
        in_specs=[vmem] * 9,
        out_specs=(vmem,) * 4,
        scratch_shapes=[
            pltpu.VMEM((LANES, chunks * LANES), f32),
            pltpu.VMEM((2, n_phi, HEAD + slots // 2, channels), f32),
            pltpu.VMEM((2, channels, tile_cols), f32),
            pltpu.VMEM((2, channels, tile_cols), f32),
            pltpu.VMEM((2, tile_rows, channels), f32),
            pltpu.VMEM((2, tile_rows, channels), f32),
            pltpu.VMEM((2, 2, tile_cols // 2, channels), f32),
            pltpu.VMEM((2, n_theta, tile_cols // 2, channels), f32),
            pltpu.VMEM((total_theta, channels), f32),
            pltpu.VMEM((n_theta, tile_rows, channels), f32),
            dma((2 * (n_phi - 1),)),
            dma((2 * (n_phi - 1),)),
            dma((4,)),
            dma((2 * n_theta,)),
            dma((n_theta,)),
            dma((n_theta,)),
            dma((4,)),
            dma((4,)),
        ],
        compiler_params=pltpu.CompilerParams(collective_id=0, has_side_effects=True, vmem_limit_bytes=16 << 20),
        name="exchange",
    )(
        *fields,
        send_row.reshape(1, slots),
        send_col.reshape(1, slots),
        send_weight.reshape(2, slots),
        send_turn.reshape(1, slots),
        send_dest.reshape(1, slots),
    )
    thetas = 0.25 * math.pi + (np.arange(total_theta) + 0.5) * d_theta
    metric = np.broadcast_to(
        (1.0 / (np.sin(thetas) * d_phi))[:, None], (total_theta, tile_cols)
    ).astype(np.float32)
    radius = R_BASE + (np.arange(levels) + 0.5) * DR_STEP
    outs = pl.pallas_call(
        functools.partial(stencil_kernel, dims),
        out_shape=tuple(jax.ShapeDtypeStruct(x.shape, f32) for x in fields),
        in_specs=[vmem] * 9 + [pl.BlockSpec(memory_space=pltpu.SMEM)],
        out_specs=(vmem,) * 4,
        compiler_params=pltpu.CompilerParams(vmem_limit_bytes=16 << 20), name="stencil",
    )(*fields, up, down, left, right, jnp.asarray(metric), jnp.asarray((1.0 / radius).astype(np.float32)))
    return tuple(
        x.reshape(like.shape) for x, like in zip(outs, (density, velocity, magnetic, pressure))
    )


def solution(mesh):
    scalar = P("patch", None, "theta", "phi")
    vector = P("patch", None, None, "theta", "phi")
    slot = P("patch", "theta", "phi", None)
    return jax.shard_map(
        functools.partial(body, mesh.shape["theta"], mesh.shape["phi"]),
        mesh=mesh,
        in_specs=(
            scalar, vector, vector, scalar, slot, slot,
            P("patch", "theta", "phi", None, None), slot, slot,
        ),
        out_specs=(scalar, vector, vector, scalar),
        check_vma=False,
    )
```

```python
import functools
import math

import jax
import jax.numpy as jnp
import numpy as np
from jax import lax
from jax.experimental import pallas as pl
from jax.experimental.pallas import tpu as pltpu
from jax.sharding import PartitionSpec as P

GAMMA = 5.0 / 3.0
R_BASE = 0.6
DR_STEP = 0.65 / 64.0
COURANT = 0.4
DIFFUSE = 0.4
MESH = pl.DeviceIdType.MESH
LANES = 128
HEAD = 8


def grid_constants(total_theta, total_phi):
    d_theta = 0.5 * math.pi / total_theta
    d_phi = 1.5 * math.pi / total_phi
    r_low = R_BASE + 0.5 * DR_STEP
    inv_r = 1.0 / DR_STEP
    inv_t = 1.0 / (r_low * d_theta)
    inv_p = 1.0 / (r_low * math.sin(0.25 * math.pi) * d_phi)
    dt_step = COURANT / (inv_r + inv_t + inv_p)
    diffusivity = DIFFUSE / (dt_step * (inv_r * inv_r + inv_t * inv_t + inv_p * inv_p))
    return (d_theta, d_phi, dt_step, diffusivity)


def split(x):
    hi = x.astype(jnp.bfloat16)
    lo = (x - hi.astype(jnp.float32)).astype(jnp.bfloat16)
    return hi, lo


def dot_nt(a, b):
    return lax.dot_general(a, b, (((1,), (1,)), ((), ())), preferred_element_type=jnp.float32)


def dot_nn(a, b):
    return jnp.dot(a, b, preferred_element_type=jnp.float32)


def exchange_kernel(
    dims, den_hbm, vel_hbm, mag_hbm, prs_hbm, srow_hbm, scol_hbm, swgt_hbm, sturn_hbm, sdest_hbm,
    up_out, down_out, left_out, right_out,
    den, vel, mag, prs, srow, scol, swgt, sturn, sdest, load_sem,
    table, gathered, rows_out, rows_in, cols_out, cols_in, lon_out, lon_in, lat_out, lat_in,
    gather_send, gather_recv, lon_send, lon_recv, lat_send, lat_recv, halo_send, halo_recv,
):
    n_theta, n_phi, levels, tile_rows, tile_cols, slots = dims
    total_phi = tile_cols * n_phi
    total_theta = tile_rows * n_theta
    channels = 8 * levels
    chunks = -(-slots // LANES)
    q = lax.axis_index("patch")
    t = lax.axis_index("theta")
    f = lax.axis_index("phi")
    other = 1 - q

    pairs = (
        (srow_hbm, srow), (scol_hbm, scol), (swgt_hbm, swgt), (sturn_hbm, sturn), (sdest_hbm, sdest),
        (den_hbm, den), (vel_hbm, vel), (mag_hbm, mag), (prs_hbm, prs),
    )
    loads = [pltpu.make_async_copy(a, b, load_sem.at[i]) for i, (a, b) in enumerate(pairs)]
    for load in loads:
        load.start()

    barrier = pltpu.get_barrier_semaphore()

    def greet(device):
        pl.semaphore_signal(barrier, inc=1, device_id=device, device_id_type=MESH)

    for d in range(1, n_phi):
        greet((q, t, lax.rem(f + d, n_phi)))
    greet((q, lax.rem(t + 1, n_theta), f))
    greet((q, lax.rem(t + n_theta - 1, n_theta), f))
    for d in range(n_theta):
        greet((other, d, f))

    table[...] = jnp.zeros_like(table)
    for load in loads[:5]:
        load.wait()
    table[0:1, :slots] = srow[...].astype(jnp.float32)
    table[1:2, :slots] = scol[...].astype(jnp.float32)
    table[2:4, :slots] = swgt[...]
    turn = sturn[...]
    table[4:5, :slots] = jnp.cos(turn)
    table[5:6, :slots] = jnp.sin(turn)
    table[6:7, :slots] = sdest[...].astype(jnp.float32)
    columns = table[...].T[:slots]
    row_s = columns[:, 0:1]
    col_s = columns[:, 1:2]
    w_row = columns[:, 2:3]
    w_col = columns[:, 3:4]
    half = slots // 2
    width = channels // 2
    fold_lane = lax.broadcasted_iota(jnp.int32, (half, channels), 1)
    lower = fold_lane < width

    def fold(x):
        return jnp.where(lower, x[:half], x[half:])

    lane = lax.broadcasted_iota(jnp.int32, (slots, tile_cols), 1).astype(jnp.float32)
    pick = jnp.where(lane == col_s, 1.0 - w_col, 0.0) + jnp.where(lane == col_s + 1.0, w_col, 0.0)
    pick_hi, pick_lo = split(pick)
    row_f = fold(row_s)
    w_row_f = fold(w_row)
    cos_f = fold(columns[:, 4:5])
    sin_f = fold(columns[:, 5:6])
    head = table[0:8, :]
    head_lane = lax.broadcasted_iota(jnp.int32, (1, LANES), 1)
    own_dest = (
        head[6:7, :LANES],
        pltpu.roll(head, chunks * LANES - half, axis=1)[6:7, :LANES],
    )
    for c in range(2):
        gathered[0, f, c:c + 1, :] = jnp.where(head_lane < half, own_dest[c], -1.0)

    def field_row(h, r):
        if h == 0:
            parts = [
                den[pl.ds(r, levels, stride=tile_rows), :],
                vel[pl.ds(r, 3 * levels, stride=tile_rows), :],
            ]
        else:
            parts = [
                mag[pl.ds(r, 3 * levels, stride=tile_rows), :],
                prs[pl.ds(r, levels, stride=tile_rows), :],
            ]
        return jnp.concatenate(parts, axis=0)

    def donors(h):
        value = jnp.zeros((half, channels), jnp.float32)
        for r in range(tile_rows):
            cells = field_row(h, r)
            if r == 0:
                rows_out[0, h * width:(h + 1) * width] = cells
            if r == tile_rows - 1:
                rows_out[1, h * width:(h + 1) * width] = cells
            hi, lo = split(jnp.concatenate([cells, cells], axis=0))
            part = dot_nt(pick_hi, hi) + (dot_nt(pick_hi, lo) + dot_nt(pick_lo, hi))
            gain = jnp.where(row_f == r, 1.0 - w_row_f, 0.0) + jnp.where(row_f + 1.0 == r, w_row_f, 0.0)
            value = value + gain * fold(part)
        comp = lax.rem(fold_lane, width) // levels + 4 * h
        first = (comp == 2) | (comp == 5)
        second = (comp == 3) | (comp == 6)
        partner = jnp.where(
            first,
            pltpu.roll(value, channels - levels, axis=1),
            pltpu.roll(value, levels, axis=1),
        )
        keep = jnp.where(first | second, cos_f, 1.0)
        mix = jnp.where(first, sin_f, jnp.where(second, -sin_f, 0.0))
        gathered[h, f, HEAD:HEAD + half, :] = keep * value + mix * partner

    def donor_ref(h, source):
        if h == 0:
            return gathered.at[0, source]
        return gathered.at[1, source, pl.ds(HEAD, half)]

    def gather_copy(h, d, source=None):
        at = f if source is None else source
        return pltpu.make_async_remote_copy(
            src_ref=donor_ref(h, at),
            dst_ref=donor_ref(h, at),
            send_sem=gather_send.at[h * (n_phi - 1) + d - 1],
            recv_sem=gather_recv.at[h * (n_phi - 1) + d - 1],
            device_id=(q, t, lax.rem(f + d, n_phi) if source is None else source),
            device_id_type=MESH,
        )

    loads[5].wait()
    loads[6].wait()
    donors(0)
    pl.semaphore_wait(barrier, n_phi - 1 + 2 + n_theta)
    for d in range(1, n_phi):
        gather_copy(0, d).start()
    loads[7].wait()
    loads[8].wait()
    donors(1)
    for d in range(1, n_phi):
        gather_copy(1, d).start()

    def row_copy(way):
        return pltpu.make_async_remote_copy(
            src_ref=rows_out.at[way],
            dst_ref=rows_in.at[way],
            send_sem=halo_send.at[way],
            recv_sem=halo_recv.at[way],
            device_id=(q, lax.rem(t + (1 if way else n_theta - 1), n_theta), f),
            device_id_type=MESH,
        )

    def col_copy(way):
        return pltpu.make_async_remote_copy(
            src_ref=cols_out.at[way],
            dst_ref=cols_in.at[way],
            send_sem=halo_send.at[2 + way],
            recv_sem=halo_recv.at[2 + way],
            device_id=(q, t, lax.rem(f + (1 if way else n_phi - 1), n_phi)),
            device_id_type=MESH,
        )

    @pl.when(t > 0)
    def _():
        row_copy(0).start()

    @pl.when(t < n_theta - 1)
    def _():
        row_copy(1).start()

    lane2 = lax.broadcasted_iota(jnp.int32, (tile_rows, channels), 1)
    low = jnp.zeros((tile_rows, channels), jnp.float32)
    high = jnp.zeros((tile_rows, channels), jnp.float32)
    for c in range(8):
        ref, base = ((den, 0), (vel, 0), (vel, 1), (vel, 2), (mag, 0), (mag, 1), (mag, 2), (prs, 0))[c]
        for k in range(levels):
            cells = ref[(base * levels + k) * tile_rows:(base * levels + k + 1) * tile_rows, :]
            hit = lane2 == c * levels + k
            low = jnp.where(hit, cells[:, 0:1], low)
            high = jnp.where(hit, cells[:, tile_cols - 1:tile_cols], high)
    cols_out[0] = low
    cols_out[1] = high

    def ids_of(count):
        return lax.broadcasted_iota(jnp.int32, (count, LANES), 0)

    ids_top = ids_of(tile_cols) + f * tile_cols
    lat_base = 2 * total_phi + jnp.where(f == 0, 0, total_theta)
    ids = jnp.concatenate(
        [ids_top, ids_top + total_phi, ids_of(total_theta) + lat_base], axis=0
    ).astype(jnp.float32)

    def place(h, source):
        folded = gathered[h, source, HEAD:HEAD + half, :]
        total = None
        for c in range(2):
            hits = jnp.where(ids == gathered[0, source, c:c + 1, :], 1.0, 0.0).astype(jnp.bfloat16)[:, :half]
            hi, lo = split(folded if c == 0 else pltpu.roll(folded, width, axis=1))
            term = dot_nn(hits, hi) + dot_nn(hits, lo)
            total = term if total is None else total + term
        return total

    @pl.when(f > 0)
    def _():
        col_copy(0).start()

    @pl.when(f < n_phi - 1)
    def _():
        col_copy(1).start()

    short = tile_cols // 2
    lon_lower = lax.broadcasted_iota(jnp.int32, (short, channels), 1) < width

    def lon_copy(h, side):
        return pltpu.make_async_remote_copy(
            src_ref=lon_out.at[h, side],
            dst_ref=lon_in.at[h, t],
            send_sem=lon_send.at[2 * h + side],
            recv_sem=lon_recv.at[h * n_theta + t],
            device_id=(other, (n_theta - 1) * side, f),
            device_id_type=MESH,
        )

    lat_parts = []
    for h in range(2):
        placed = place(h, f)
        for d in range(1, n_phi):
            source = lax.rem(f + n_phi - d, n_phi)
            gather_copy(h, d, source).wait_recv()
            placed = placed + place(h, source)
        for side in range(2):
            base = side * tile_cols
            lon_out[h, side] = jnp.where(
                lon_lower,
                placed[base:base + short],
                pltpu.roll(placed[base + short:base + tile_cols], width, axis=1),
            )
        lat_parts.append(placed[2 * tile_cols:])
        lon_copy(h, 0).start()
        lon_copy(h, 1).start()
    lat_lower = lax.broadcasted_iota(jnp.int32, (total_theta, channels), 1) < width
    lat_out[...] = jnp.where(lat_lower, lat_parts[0], pltpu.roll(lat_parts[1], width, axis=1))

    def lat_copy(d):
        return pltpu.make_async_remote_copy(
            src_ref=lat_out.at[pl.ds(d * tile_rows, tile_rows)],
            dst_ref=lat_in.at[t],
            send_sem=lat_send.at[d],
            recv_sem=lat_recv.at[t],
            device_id=(other, d, f),
            device_id_type=MESH,
        )

    at_side = (f == 0) | (f == n_phi - 1)
    at_end = (t == 0) | (t == n_theta - 1)

    @pl.when(at_side)
    def _():
        for d in range(n_theta):
            lat_copy(d).start()

    @pl.when(t > 0)
    def _():
        row_copy(1).wait_recv()
        up_out[...] = rows_in[1]

    @pl.when(t < n_theta - 1)
    def _():
        row_copy(0).wait_recv()
        down_out[...] = rows_in[0]

    @pl.when(f > 0)
    def _():
        col_copy(1).wait_recv()
        left_out[...] = cols_in[1]

    @pl.when(f < n_phi - 1)
    def _():
        col_copy(0).wait_recv()
        right_out[...] = cols_in[0]

    @pl.when(at_end)
    def _():
        sums = []
        for h in range(2):
            total = None
            for s in range(n_theta):
                pltpu.make_async_remote_copy(
                    src_ref=lon_in.at[h, s],
                    dst_ref=lon_in.at[h, s],
                    send_sem=lon_send.at[0],
                    recv_sem=lon_recv.at[h * n_theta + s],
                    device_id=(other, s, f),
                    device_id_type=MESH,
                ).wait_recv()
                total = lon_in[h, s] if total is None else total + lon_in[h, s]
            sums.append(total)
        total = jnp.concatenate(
            [
                jnp.where(lon_lower, sums[0], pltpu.roll(sums[1], width, axis=1)),
                jnp.where(lon_lower, pltpu.roll(sums[0], width, axis=1), sums[1]),
            ],
            axis=0,
        )
        total = total.T

        @pl.when(t == 0)
        def _():
            up_out[...] = total

        @pl.when(t == n_theta - 1)
        def _():
            down_out[...] = total

    @pl.when(at_side)
    def _():
        for s in range(n_theta):
            pltpu.make_async_remote_copy(
                src_ref=lat_in.at[s],
                dst_ref=lat_in.at[s],
                send_sem=lat_send.at[0],
                recv_sem=lat_recv.at[s],
                device_id=(other, s, f),
                device_id_type=MESH,
            ).wait_recv()
        total = lat_in[0]
        for s in range(1, n_theta):
            total = total + lat_in[s]

        @pl.when(f == 0)
        def _():
            left_out[...] = total

        @pl.when(f == n_phi - 1)
        def _():
            right_out[...] = total

    for h in range(2):
        for d in range(1, n_phi):
            gather_copy(h, d).wait_send()
        lon_copy(h, 0).wait_send()
        lon_copy(h, 1).wait_send()

    @pl.when(at_side)
    def _():
        for d in range(n_theta):
            lat_copy(d).wait_send()

    @pl.when(t > 0)
    def _():
        row_copy(0).wait_send()

    @pl.when(t < n_theta - 1)
    def _():
        row_copy(1).wait_send()

    @pl.when(f > 0)
    def _():
        col_copy(0).wait_send()

    @pl.when(f < n_phi - 1)
    def _():
        col_copy(1).wait_send()


def stencil_kernel(
    dims, parts, den_hbm, vel_hbm, mag_hbm, prs_hbm, up_hbm, down_hbm, left_hbm, right_hbm, metric_hbm,
    inv_radius, den_out, vel_out, mag_out, prs_out,
    den, vel, mag, prs, up, down, left, right, metric, new_den, new_vel, new_mag, new_prs,
    ghost_sem, load_sem, store_sem,
):
    n_theta, n_phi, levels, rows, cols, _ = dims
    d_theta, _, dt_step, diffusivity = grid_constants(rows * n_theta, cols * n_phi)
    g_r = 1.0 / DR_STEP
    span = levels // parts
    first_row = pl.multiple_of(lax.axis_index("theta") * rows, rows)
    ghosts = [
        pltpu.make_async_copy(a, b, ghost_sem.at[i])
        for i, (a, b) in enumerate(
            (
                (up_hbm, up), (down_hbm, down), (left_hbm, left), (right_hbm, right),
                (metric_hbm.at[pl.ds(first_row, rows)], metric),
            )
        )
    ]

    def pieces(sources, targets, sems, part):
        rows_of = pl.ds(part * span * rows, span * rows)
        return [
            pltpu.make_async_copy(a.at[:, rows_of], b.at[:, rows_of], sems.at[part, i])
            for i, (a, b) in enumerate(zip(sources, targets))
        ]

    loads = [
        pieces((den_hbm, vel_hbm, mag_hbm, prs_hbm), (den, vel, mag, prs), load_sem, part)
        for part in range(parts)
    ]
    stores = [
        pieces((new_den, new_vel, new_mag, new_prs), (den_out, vel_out, mag_out, prs_out), store_sem, part)
        for part in range(parts)
    ]
    for copy in loads[0] + ghosts:
        copy.start()
    for part in range(1, parts):
        for copy in loads[part]:
            copy.start()
    for copy in ghosts + loads[0]:
        copy.wait()
    lon_row = metric[...]
    row_id = lax.broadcasted_iota(jnp.int32, (rows, cols), 0)
    col_id = lax.broadcasted_iota(jnp.int32, (rows, cols), 1)
    at_up = row_id == 0
    at_down = row_id == rows - 1
    at_left = col_id == 0
    at_right = col_id == cols - 1
    sources = ((den, 0), (vel, 0), (vel, 1), (vel, 2), (mag, 0), (mag, 1), (mag, 2), (prs, 0))
    channels = 8 * levels

    def level(k, carry):
        inv_rk = inv_radius[k]
        g_t = inv_rk * (1.0 / d_theta)
        g_p = lon_row * inv_rk
        half_r = 0.5 * g_r
        half_t = 0.5 * g_t
        half_p = 0.5 * g_p
        below = jnp.maximum(k - 1, 0)
        above = jnp.minimum(k + 1, levels - 1)

        def load(c, kk):
            ref, base = sources[c]
            return ref[base, pl.ds(pl.multiple_of(kk * rows, rows), rows), :]

        mid = [load(c, k) for c in range(8)]
        r_lo = [load(c, below) for c in range(8)]
        r_hi = [load(c, above) for c in range(8)]
        left_all = left[...]
        right_all = right[...]
        t_lo, t_hi, p_lo, p_hi = [], [], [], []
        for c in range(8):
            u = mid[c]
            ck = c * levels + k
            t_lo.append(jnp.where(at_up, up[pl.ds(ck, 1), :], pltpu.roll(u, 1, axis=0)))
            t_hi.append(jnp.where(at_down, down[pl.ds(ck, 1), :], pltpu.roll(u, rows - 1, axis=0)))
            p_lo.append(
                jnp.where(at_left, pltpu.roll(left_all, channels - ck, axis=1), pltpu.roll(u, 1, axis=1))
            )
            p_hi.append(
                jnp.where(
                    at_right,
                    pltpu.roll(right_all, channels - 1 - ck, axis=1),
                    pltpu.roll(u, cols - 1, axis=1),
                )
            )

        def dr(c):
            return (r_hi[c] - r_lo[c]) * half_r

        def dth(c):
            return (t_hi[c] - t_lo[c]) * half_t

        def dp(c):
            return (p_hi[c] - p_lo[c]) * half_p

        rr = g_r * g_r
        tt = g_t * g_t
        pp = g_p * g_p

        def laplace(c):
            centre = 2.0 * mid[c]
            return (
                (r_hi[c] + r_lo[c] - centre) * rr
                + (t_hi[c] + t_lo[c] - centre) * tt
                + (p_hi[c] + p_lo[c] - centre) * pp
            )

        v_r, v_t, v_p = mid[1], mid[2], mid[3]
        b_r, b_t, b_p = mid[4], mid[5], mid[6]
        rho, press = mid[0], mid[7]
        div_mom = (
            (r_hi[0] * r_hi[1] - r_lo[0] * r_lo[1]) * half_r
            + (t_hi[0] * t_hi[2] - t_lo[0] * t_lo[2]) * half_t
            + (p_hi[0] * p_hi[3] - p_lo[0] * p_lo[3]) * half_p
        )

        def put(ref, base, x):
            ref[base, pl.ds(pl.multiple_of(k * rows, rows), rows), :] = x

        put(new_den, 0, rho - dt_step * div_mom)

        grads = [(dr(c), dth(c), dp(c)) for c in range(1, 4)]
        inv_rho = 1.0 / rho
        j_r = dth(6) - dp(5)
        j_t = dp(4) - dr(6)
        j_p = dr(5) - dth(4)
        lorentz = (j_t * b_p - j_p * b_t, j_p * b_r - j_r * b_p, j_r * b_t - j_t * b_r)
        p_grad = (dr(7), dth(7), dp(7))
        for i in range(3):
            g = grads[i]
            carried = v_r * g[0] + v_t * g[1] + v_p * g[2]
            put(
                new_vel, i,
                mid[1 + i]
                + dt_step
                * ((lorentz[i] - p_grad[i]) * inv_rho - carried + diffusivity * laplace(1 + i)),
            )

        def emf(s, i):
            a, b = ((2, 3), (3, 1), (1, 2))[i]
            return s[a] * s[b + 3] - s[b] * s[a + 3]

        def diff(lo, hi, i):
            return emf(hi, i) - emf(lo, i)

        curl = (
            diff(t_lo, t_hi, 2) * half_t - diff(p_lo, p_hi, 1) * half_p,
            diff(p_lo, p_hi, 0) * half_p - diff(r_lo, r_hi, 2) * half_r,
            diff(r_lo, r_hi, 1) * half_r - diff(t_lo, t_hi, 0) * half_t,
        )
        for i in range(3):
            put(new_mag, i, mid[4 + i] + dt_step * (curl[i] + diffusivity * laplace(4 + i)))
        div_flow = grads[0][0] + grads[1][1] + grads[2][2]
        carried = v_r * p_grad[0] + v_t * p_grad[1] + v_p * p_grad[2]
        put(
            new_prs, 0,
            press + dt_step * (diffusivity * laplace(7) - carried - GAMMA * press * div_flow),
        )
        return carry

    for part in range(parts):
        if part + 1 < parts:
            for copy in loads[part + 1]:
                copy.wait()
        lax.fori_loop(part * span, (part + 1) * span, level, 0)
        for copy in stores[part]:
            copy.start()
    for part in range(parts):
        for copy in stores[part]:
            copy.wait()


def body(
    n_theta, n_phi,
    density, velocity, magnetic, pressure, send_row, send_col, send_weight, send_turn, send_dest,
):
    levels, tile_rows, tile_cols = density.shape[1:]
    slots = send_row.shape[-1]
    dims = (n_theta, n_phi, levels, tile_rows, tile_cols, slots)
    channels = 8 * levels
    chunks = -(-slots // LANES)
    total_theta = n_theta * tile_rows
    _, d_phi, _, _ = grid_constants(total_theta, n_phi * tile_cols)
    d_theta = 0.5 * math.pi / total_theta
    fields = [x.reshape(-1, tile_cols) for x in (density, velocity, magnetic, pressure)]
    vmem = pl.BlockSpec(memory_space=pltpu.VMEM)
    f32 = jnp.float32
    dma = pltpu.SemaphoreType.DMA
    tile_row = jax.ShapeDtypeStruct((channels, tile_cols), f32)
    tile_col = jax.ShapeDtypeStruct((tile_rows, channels), f32)
    up, down, left, right = pl.pallas_call(
        functools.partial(exchange_kernel, dims),
        out_shape=(tile_row, tile_row, tile_col, tile_col),
        in_specs=[pl.BlockSpec(memory_space=pl.ANY)] * 9,
        out_specs=(vmem,) * 4,
        scratch_shapes=[
            *(pltpu.VMEM(x.shape, f32) for x in fields),
            pltpu.VMEM((1, slots), jnp.int32),
            pltpu.VMEM((1, slots), jnp.int32),
            pltpu.VMEM((2, slots), f32),
            pltpu.VMEM((1, slots), f32),
            pltpu.VMEM((1, slots), jnp.int32),
            dma((9,)),
            pltpu.VMEM((LANES, chunks * LANES), f32),
            pltpu.VMEM((2, n_phi, HEAD + slots // 2, channels), f32),
            pltpu.VMEM((2, channels, tile_cols), f32),
            pltpu.VMEM((2, channels, tile_cols), f32),
            pltpu.VMEM((2, tile_rows, channels), f32),
            pltpu.VMEM((2, tile_rows, channels), f32),
            pltpu.VMEM((2, 2, tile_cols // 2, channels), f32),
            pltpu.VMEM((2, n_theta, tile_cols // 2, channels), f32),
            pltpu.VMEM((total_theta, channels), f32),
            pltpu.VMEM((n_theta, tile_rows, channels), f32),
            dma((2 * (n_phi - 1),)),
            dma((2 * (n_phi - 1),)),
            dma((4,)),
            dma((2 * n_theta,)),
            dma((n_theta,)),
            dma((n_theta,)),
            dma((4,)),
            dma((4,)),
        ],
        compiler_params=pltpu.CompilerParams(collective_id=0, has_side_effects=True),
        name="exchange",
    )(
        *fields,
        send_row.reshape(1, slots),
        send_col.reshape(1, slots),
        send_weight.reshape(2, slots),
        send_turn.reshape(1, slots),
        send_dest.reshape(1, slots),
    )
    thetas = 0.25 * math.pi + (np.arange(total_theta) + 0.5) * d_theta
    metric = np.broadcast_to(
        (1.0 / (np.sin(thetas) * d_phi))[:, None], (total_theta, tile_cols)
    ).astype(np.float32)
    radius = R_BASE + (np.arange(levels) + 0.5) * DR_STEP
    stacked = [x.reshape(-1, levels * tile_rows, tile_cols) for x in (density, velocity, magnetic, pressure)]
    parts = 4 if levels % 4 == 0 else 1
    hbm = pl.BlockSpec(memory_space=pl.ANY)
    outs = pl.pallas_call(
        functools.partial(stencil_kernel, dims, parts),
        out_shape=tuple(jax.ShapeDtypeStruct(x.shape, f32) for x in stacked),
        in_specs=[hbm] * 9 + [pl.BlockSpec(memory_space=pltpu.SMEM)],
        out_specs=(hbm,) * 4,
        scratch_shapes=[
            *(pltpu.VMEM(x.shape, f32) for x in stacked),
            pltpu.VMEM((channels, tile_cols), f32),
            pltpu.VMEM((channels, tile_cols), f32),
            pltpu.VMEM((tile_rows, channels), f32),
            pltpu.VMEM((tile_rows, channels), f32),
            pltpu.VMEM((tile_rows, tile_cols), f32),
            *(pltpu.VMEM(x.shape, f32) for x in stacked),
            dma((5,)),
            dma((parts, 4)),
            dma((parts, 4)),
        ],
        name="stencil",
    )(*stacked, up, down, left, right, jnp.asarray(metric), jnp.asarray((1.0 / radius).astype(np.float32)))
    return tuple(
        x.reshape(like.shape) for x, like in zip(outs, (density, velocity, magnetic, pressure))
    )


def solution(mesh):
    scalar = P("patch", None, "theta", "phi")
    vector = P("patch", None, None, "theta", "phi")
    slot = P("patch", "theta", "phi", None)
    return jax.shard_map(
        functools.partial(body, mesh.shape["theta"], mesh.shape["phi"]),
        mesh=mesh,
        in_specs=(
            scalar, vector, vector, scalar, slot, slot,
            P("patch", "theta", "phi", None, None), slot, slot,
        ),
        out_specs=(scalar, vector, vector, scalar),
        check_vma=False,
    )
```
